32 devices in a mesh: vert: 4 (over y, x), feat: 8 (over z, core).
Axes of the slice: x: 2, y: 2, z: 4, core: 2. Of those that a mesh axis runs over, the one named last changes fastest.
Arguments:
- features: bfloat16 [32768, 256], P('vert', 'feat'), may hold values from -6 to 6
- tiles: bfloat16 [256, 16, 128, 128], P('vert'), may hold values from -0.1875 to 0.1875
- tile_cols: int32 [256, 16], P('vert'), may hold values from 0 to 79
- tile_count: int32 [256], P('vert'), may hold values from 1 to 16, as said below
- send_list: int32 [4, 4, 4], P('vert'), may hold values from 0 to 63
- weight: bfloat16 [256, 256], replicated, may hold values from -0.375 to 0.375
- bias: float32 [256], replicated, may hold values from -3 to 3
Outputs:
- node_out: bfloat16 [32768, 256], P(('vert', 'feat'))
The draws below stay inside these ranges and needn't reach their ends.
Inputs may be any that keep to these rules, and one draw needn't show every extreme that they name: Row block r uses tile places 0 to tile_count[r] - 1; in every draw some row block uses all 16.
All inputs are finite; a program needn't handle non-finite values.
Results may differ from the reference program's by a relative error of at most 0.0044.
Values may be sent and summed in bfloat16 or wider, within the bound.
A program may use at most 128 MiB of HBM per device.

```python
import jax
import jax.numpy as jnp
from jax import lax

F = 256
BLK = 128
K = 16
SLOTS = 4
RB_DEV = 64
NRB = 256
NV = 32768
N_VERT = 4


def draw_tile_count(key, part):
    total = RB_DEV * N_VERT
    row_index = jnp.arange(total, dtype=jnp.int32)
    rank = row_index // RB_DEV
    ceiling = 1 + (K - 1) * (rank + 1) // N_VERT
    picks = jax.random.randint(key, (total,), 0, 1 << 20)
    counts = 1 + picks % ceiling
    chosen = jax.random.randint(jax.random.fold_in(key, 7), (), 0, total)
    return jnp.where(row_index == chosen, K, counts).astype(jnp.int32)


def with_ends(values, rng, least, top_value):
    spot = [jax.random.randint(jax.random.fold_in(rng, axis), (), 0, length) for axis, length in enumerate(values.shape)]
    longest = values.shape.index(max(values.shape))
    next_to = spot[:longest] + [(spot[longest] + 1) % values.shape[longest]] + spot[longest + 1:]
    return values.at[tuple(spot)].set(least).at[tuple(next_to)].set(top_value)


def block_levels(stream_key, dims, split, smallest, top_value):
    gain, own = 1.0, jax.random.fold_in(stream_key, 6)
    for dim, parts in split:
        steps = jnp.exp(jax.random.uniform(jax.random.fold_in(own, dim), (parts,), jnp.float32, smallest / len(split), top_value / len(split)))
        gain = gain * jnp.repeat(steps, dims[dim] // parts).reshape([-1 if axis == dim else 1 for axis in range(len(dims))])
    return gain


def scatter_about(rng, shape, width, reach, cuts=(), held_as=jnp.bfloat16):
    array = jax.random.normal(rng, shape, jnp.float32) * width
    if len(cuts) > 0:
        array = block_levels(rng, shape, cuts, -0.22, 0.18) * array
    return jnp.clip(array, min=-reach, max=reach).astype(held_as)


def setup_inputs(seed: int = 0) -> dict:
    streams_of = jax.random.split(jax.random.key(seed), 8)
    features = scatter_about(streams_of[0], (NV, F), 1.0, 6.0, ((0, 4), (1, 8)))
    tiles = scatter_about(streams_of[1], (NRB, K, BLK, BLK), (BLK * K // 2) ** -0.5, 0.1875, ((0, 4),))
    tile_cols = with_ends(jax.random.randint(streams_of[2], (NRB, K), 0, RB_DEV + N_VERT * SLOTS), jax.random.fold_in(streams_of[2], 1), 0, (RB_DEV + N_VERT * SLOTS) - 1).astype(jnp.int32)
    tile_count = draw_tile_count(jax.random.fold_in(streams_of[7], 71), 0)
    send_list = with_ends(jax.random.randint(streams_of[4], (N_VERT, N_VERT, SLOTS), 0, RB_DEV), jax.random.fold_in(streams_of[4], 1), 0, RB_DEV - 1).astype(jnp.int32)
    weight = scatter_about(streams_of[5], (F, F), F ** -0.5, 0.375)
    bias = scatter_about(streams_of[6], (F,), 0.5, 3.0, (), jnp.float32)
    return dict(features=features, tiles=tiles, tile_cols=tile_cols, tile_count=tile_count, send_list=send_list, weight=weight, bias=bias)


def reference(features, tiles, tile_cols, tile_count, send_list, weight, bias):
    row_owner = jnp.arange(RB_DEV * N_VERT, dtype=jnp.int32) // RB_DEV
    is_local = tile_cols < RB_DEV
    halo_slot = jnp.maximum(tile_cols - RB_DEV, 0)
    source = (halo_slot // SLOTS).astype(jnp.int32)
    position = (halo_slot % SLOTS).astype(jnp.int32)
    sent_block = send_list[source, row_owner[:, None], position]
    column = jnp.where(is_local, row_owner[:, None] * RB_DEV + tile_cols, source * RB_DEV + sent_block).astype(jnp.int32)
    blocks = features.reshape(RB_DEV * N_VERT, BLK, F)
    is_live = jnp.arange(K, dtype=jnp.int32)[None, :] < tile_count[:, None]

    def one_block(block_item):
        tile_row, col_row, live_row = block_item
        picked = blocks[col_row].astype(jnp.float32)
        products = jnp.einsum("kij,kjc->kic", tile_row.astype(jnp.float32), picked)
        kept = jnp.where(live_row[:, None, None], products, jnp.float32(0.0))
        return jnp.sum(kept, axis=0).astype(jnp.bfloat16)

    aggregated = lax.map(one_block, (tiles, column, is_live)).reshape(RB_DEV * N_VERT * BLK, F)
    mixed_rows = jnp.dot(aggregated, weight, preferred_element_type=jnp.float32) + bias
    return jnp.maximum(mixed_rows, jnp.float32(0.0)).astype(jnp.bfloat16)
```

```python
import functools

import jax
import jax.numpy as jnp
from jax import lax
from jax.experimental import pallas as pl
from jax.experimental.pallas import tpu as pltpu
from jax.sharding import PartitionSpec as P

MESH = pl.DeviceIdType.MESH
GROUP = 4


def visiting_order(chip, chips):
    others = [other for other in range(chips) if other != chip]
    if 0 < chip < chips // 2:
        others.remove(chip + 1)
        others.insert(0, chip + 1)
    elif chip == chips - 1 and chips > 2:
        others[-2:] = others[:-3:-1]
    return others + [chip]


def order_code(chip, chips):
    codes = [
        sum(other * chips**at for at, other in enumerate(visiting_order(one, chips)))
        for one in range(chips)
    ]
    code = codes[0]
    for one in range(1, chips):
        code = jnp.where(chip == one, codes[one], code)
    return code


def exchange_kernel(
    dims, cols_in, count_in, send_in, features, tiles, gathered,
    cols, count, send, table_sem, extended, local, outgoing, landed, hidden, pages,
    load_sem, page_sem, halo_send, halo_recv, full_send, full_recv, above, below,
):
    verts, feats, cores, blocks, depth, edge, width, slots, group = dims
    chips = feats // cores
    per_dest = blocks // feats
    parts = per_dest // group
    span = group * edge
    dead = blocks + verts * slots
    vert = lax.axis_index("vert")
    feat = lax.axis_index("feat")
    chip, core = feat // cores, feat % cores

    def next_code(at, code):
        return jnp.where(at % cores == cores - 1, code // chips, code)

    def dest_of(at, code):
        away = at % cores
        mine = code % chips == chip
        return (code % chips) * cores + (core + away + jnp.where(mine, 1, 0)) % cores

    def page_copy(at, code, part):
        first = dest_of(at, code) * per_dest + part * group
        return pltpu.make_async_copy(
            tiles.at[pl.ds(first, group)], pages.at[at, part], page_sem.at[at, part]
        )

    local_copy = pltpu.make_async_copy(features, local, load_sem)
    local_copy.start()
    tables = [
        pltpu.make_async_copy(source, target, table_sem.at[at])
        for at, (source, target) in enumerate(((send_in, send), (cols_in, cols), (count_in, count)))
    ]
    for table in tables:
        table.start()
    barrier = pltpu.get_barrier_semaphore()
    for step in range(1, verts):
        pl.semaphore_signal(
            barrier, inc=1, device_id=((vert + step) % verts, feat), device_id_type=MESH
        )

    def greet(other):
        pl.semaphore_signal(barrier, inc=1, device_id=(vert, other), device_id_type=MESH)

    for step in range(1, cores):
        greet(chip * cores + (core + step) % cores)

    @pl.when(chip > 0)
    def _():
        for other in range(cores):
            greet((chip - 1) * cores + other)

    @pl.when(chip < chips - 1)
    def _():
        for other in range(cores):
            greet((chip + 1) * cores + other)

    code = order_code(chip, chips)
    walk = code
    for at in range(feats):
        for part in range(parts):
            page_copy(at, walk, part).start()
        walk = next_code(at, walk)
    extended[dead] = jnp.zeros((width, edge), jnp.bfloat16)
    tables[0].wait()
    local_copy.wait()
    for block in range(blocks):
        extended[block] = local[:, block * edge : (block + 1) * edge]
    for step in range(verts):
        peer = (vert + step) % verts
        for slot in range(slots):
            outgoing[step, slot] = extended[send[0, peer, slot]]
    neighbours = jnp.where(chip > 0, 1, 0) + jnp.where(chip < chips - 1, 1, 0)
    pl.semaphore_wait(barrier, verts + cores - 2 + cores * neighbours)
    halos = []
    for step in range(1, verts):
        halos.append(
            pltpu.make_async_remote_copy(
                src_ref=outgoing.at[step],
                dst_ref=landed.at[step],
                send_sem=halo_send.at[step],
                recv_sem=halo_recv.at[step],
                device_id=((vert + step) % verts, feat),
                device_id_type=MESH,
            )
        )
    for halo in halos[::-1]:
        halo.start()

    for far in range(2, chips):

        @pl.when((chip >= 1) & (chip + far - 1 <= chips - 1))
        def _():
            if far > 2:
                pl.semaphore_wait(above.at[far - 1], 1)
            pl.semaphore_signal(
                above.at[far], inc=1, device_id=(vert, feat - cores), device_id_type=MESH
            )

        @pl.when((chip <= chips - 2) & (chip - far + 1 >= 0))
        def _():
            if far > 2:
                pl.semaphore_wait(below.at[far - 1], 1)
            pl.semaphore_signal(
                below.at[far], inc=1, device_id=(vert, feat + cores), device_id_type=MESH
            )

    for table in tables[1:]:
        table.wait()
    extended[pl.ds(blocks + vert * slots, slots)] = outgoing[0]
    for step in range(1, verts):
        halos[step - 1].wait()
        source = (vert + verts - step) % verts
        extended[pl.ds(blocks + source * slots, slots)] = landed[step]

    mine = pl.ds(pl.multiple_of(feat * width, width), width)

    def full_copy(at, code):
        return pltpu.make_async_remote_copy(
            src_ref=hidden.at[at],
            dst_ref=gathered.at[mine],
            send_sem=full_send.at[at],
            recv_sem=full_recv.at[feat],
            device_id=(vert, dest_of(at, code)),
            device_id_type=MESH,
        )

    def aggregate(at, code):
        towards = code % chips
        first = dest_of(at, code) * per_dest
        for part in range(parts):
            page_copy(at, code, part).wait()
        for row in range(per_dest):
            picked = []
            live = count[first + row]
            for place in range(depth):
                column = jnp.where(place < live, cols[place, first + row], dead)
                picked.append(extended[column])
            page = jnp.concatenate(
                [pages[at, row // group, row % group, place] for place in range(depth)], axis=1
            )
            total = lax.dot_general(
                page,
                jnp.concatenate(picked, axis=1),
                (((1,), (1,)), ((), ())),
                preferred_element_type=jnp.float32,
            )
            hidden[at, :, row * edge : (row + 1) * edge] = total.T.astype(jnp.bfloat16)

        @pl.when((at % cores == 0) & (chip == 0) & (towards >= 2))
        def _():
            pl.semaphore_wait(above.at[towards], 1)

        @pl.when((at % cores == 0) & (chip == chips - 1) & (towards <= chips - 3))
        def _():
            pl.semaphore_wait(below.at[chips - 1 - towards], 1)

        @pl.when(at < feats - 1)
        def _():
            full_copy(at, code).start()

        return next_code(at, code)

    lax.fori_loop(0, feats, aggregate, code)
    gathered[mine, :] = hidden[feats - 1]

    def finish(at, code):
        full_copy(at, code).wait_send()
        return next_code(at, code)

    lax.fori_loop(0, feats - 1, finish, code)

    def arrive(step, carry):
        source = (feat + step) % feats
        pltpu.make_async_remote_copy(
            src_ref=hidden.at[0],
            dst_ref=gathered.at[pl.ds(pl.multiple_of(source * width, width), width)],
            send_sem=full_send.at[0],
            recv_sem=full_recv.at[source],
            device_id=(vert, source),
            device_id_type=MESH,
        ).wait_recv()
        return carry

    lax.fori_loop(1, feats, arrive, 0)


def per_device(features, tiles, tile_cols, tile_count, send_list, weight, bias):
    blocks, depth, edge = tiles.shape[:3]
    width = features.shape[1]
    verts, feats = lax.axis_size("vert"), lax.axis_size("feat")
    cores = 2 if feats % 2 == 0 else 1
    slots = send_list.shape[2]
    per_dest = blocks // feats
    group = min(GROUP, per_dest)
    parts = per_dest // group
    rows = per_dest * edge
    dead = blocks + verts * slots
    chips = feats // cores
    dims = (verts, feats, cores, blocks, depth, edge, width, slots, group)
    held = [
        pltpu.VMEM((dead + 1, width, edge), jnp.bfloat16),
        pltpu.VMEM((width, blocks * edge), jnp.bfloat16),
        pltpu.VMEM((verts, slots, width, edge), jnp.bfloat16),
        pltpu.VMEM((verts, slots, width, edge), jnp.bfloat16),
        pltpu.VMEM((feats, width, rows), jnp.bfloat16),
        pltpu.VMEM((feats, parts, group, depth, edge, edge), jnp.bfloat16),
    ]
    gathered = pl.pallas_call(
        functools.partial(exchange_kernel, dims),
        out_shape=jax.ShapeDtypeStruct((feats * width, rows), jnp.bfloat16),
        in_specs=[pl.BlockSpec(memory_space=pltpu.HBM)] * 5,
        out_specs=pl.BlockSpec(memory_space=pltpu.VMEM),
        scratch_shapes=[
            pltpu.SMEM((depth, blocks), jnp.int32),
            pltpu.SMEM((blocks,), jnp.int32),
            pltpu.SMEM(send_list.shape, jnp.int32),
            pltpu.SemaphoreType.DMA((3,)),
            *held,
            pltpu.SemaphoreType.DMA,
            pltpu.SemaphoreType.DMA((feats, parts)),
            pltpu.SemaphoreType.DMA((verts,)),
            pltpu.SemaphoreType.DMA((verts,)),
            pltpu.SemaphoreType.DMA((feats,)),
            pltpu.SemaphoreType.DMA((feats,)),
            pltpu.SemaphoreType.REGULAR((chips + 1,)),
            pltpu.SemaphoreType.REGULAR((chips + 1,)),
        ],
        compiler_params=pltpu.CompilerParams(
            collective_id=0, has_side_effects=True, vmem_limit_bytes=60 * 1024 * 1024
        ),
    )(tile_cols.T, tile_count, send_list, features.T, tiles)
    mixed_rows = lax.dot_general(
        gathered, weight, (((0,), (0,)), ((), ())), preferred_element_type=jnp.float32
    )
    return jnp.maximum(mixed_rows + bias, jnp.float32(0.0)).astype(jnp.bfloat16)


def solution(mesh):
    return jax.shard_map(
        per_device,
        mesh=mesh,
        in_specs=(
            P("vert", "feat"),
            P("vert", None, None, None),
            P("vert", None),
            P("vert"),
            P("vert", None, None),
            P(),
            P(),
        ),
        out_specs=P(("vert", "feat"), None),
        check_vma=False,
    )
```

```python
import functools

import jax
import jax.numpy as jnp
from jax import lax
from jax.experimental import pallas as pl
from jax.experimental.pallas import tpu as pltpu
from jax.sharding import PartitionSpec as P

MESH = pl.DeviceIdType.MESH
GROUP = 4


def visiting_order(chip, chips):
    half = chips // 2
    upper = list(range(chips - 1, chip, -1))
    if chip < half or half == 0:
        return list(range(chip - 1, -1, -1)) + upper + [chip]
    far = list(range(half))
    if chip == half:
        far = far[::-1]
    return list(range(chip - 1, half - 1, -1)) + far + upper + [chip]


def order_code(chip, chips):
    codes = [
        sum(other * chips**at for at, other in enumerate(visiting_order(one, chips)))
        for one in range(chips)
    ]
    code = codes[0]
    for one in range(1, chips):
        code = jnp.where(chip == one, codes[one], code)
    return code


def exchange_kernel(
    dims, cols_in, count_in, send_in, features, tiles, weight_in, bias_in, out,
    cols, count, send, table_sem, extended, local, outgoing, landed, hidden, pages,
    gathered, weight, bias, load_sem, page_sem, halo_send, halo_recv, full_send, full_recv,
    above, below,
):
    verts, feats, cores, blocks, depth, edge, width, slots, group = dims
    chips = feats // cores
    per_dest = blocks // feats
    parts = per_dest // group
    span = group * edge
    dead = blocks + verts * slots
    vert = lax.axis_index("vert")
    feat = lax.axis_index("feat")
    chip, core = feat // cores, feat % cores

    def next_code(at, code):
        return jnp.where(at % cores == cores - 1, code // chips, code)

    def dest_of(at, code):
        away = at % cores
        mine = code % chips == chip
        return (code % chips) * cores + (core + away + jnp.where(mine, 1, 0)) % cores

    def page_copy(at, code, part):
        first = dest_of(at, code) * per_dest + part * group
        return pltpu.make_async_copy(
            tiles.at[pl.ds(first, group)], pages.at[at, part], page_sem.at[at, part]
        )

    local_copy = pltpu.make_async_copy(features, local, load_sem)
    local_copy.start()
    sources = (send_in, cols_in, count_in, weight_in, bias_in)
    tables = [
        pltpu.make_async_copy(source, target, table_sem.at[at])
        for at, (source, target) in enumerate(zip(sources, (send, cols, count, weight, bias)))
    ]
    for table in tables[:3]:
        table.start()
    barrier = pltpu.get_barrier_semaphore()
    for step in range(1, verts):
        pl.semaphore_signal(
            barrier, inc=1, device_id=((vert + step) % verts, feat), device_id_type=MESH
        )

    def greet(other):
        pl.semaphore_signal(barrier, inc=1, device_id=(vert, other), device_id_type=MESH)

    for step in range(1, cores):
        greet(chip * cores + (core + step) % cores)

    @pl.when(chip < chips - 1)
    def _():
        for other in range(cores):
            greet((chip + 1) * cores + other)

    code = order_code(chip, chips)
    walk = code
    for at in range(feats):
        for part in range(parts):
            page_copy(at, walk, part).start()
        walk = next_code(at, walk)
    for table in tables[3:]:
        table.start()
    extended[dead] = jnp.zeros((width, edge), jnp.bfloat16)
    tables[0].wait()
    local_copy.wait()
    for block in range(blocks):
        extended[block] = local[:, block * edge : (block + 1) * edge]
    for step in range(verts):
        peer = (vert + step) % verts
        for slot in range(slots):
            outgoing[step, slot] = extended[send[0, peer, slot]]
    pl.semaphore_wait(barrier, verts + cores - 2 + cores * jnp.where(chip > 0, 1, 0))

    def halo(step):
        return pltpu.make_async_remote_copy(
            src_ref=outgoing.at[step],
            dst_ref=landed.at[step],
            send_sem=halo_send.at[step],
            recv_sem=halo_recv.at[step],
            device_id=((vert + step) % verts, feat),
            device_id_type=MESH,
        )

    for peer in range(verts):

        @pl.when(peer != vert)
        def _():
            halo((peer + verts - vert) % verts).start()

    def tell(sem, other):
        pl.semaphore_signal(sem, inc=1, device_id=(vert, other), device_id_type=MESH)

    @pl.when(chip > 0)
    def _():
        tell(above.at[1], feat - cores)

    @pl.when(chip < chips - 1)
    def _():
        pl.semaphore_wait(above.at[1], 1)

    for far in range(2, chips):

        @pl.when((chip >= 1) & (chip + far - 1 <= chips - 1))
        def _():
            if far > 2:
                pl.semaphore_wait(above.at[far - 1], 1)
            tell(above.at[far], feat - cores)

        @pl.when((chip <= chips - 2) & (chip - far + 1 >= 0))
        def _():
            if far > 2:
                pl.semaphore_wait(below.at[far - 1], 1)
            tell(below.at[far], feat + cores)

    for table in tables[1:3]:
        table.wait()
    extended[pl.ds(blocks + vert * slots, slots)] = outgoing[0]
    for step in range(1, verts):
        halo(step).wait()
        source = (vert + verts - step) % verts
        extended[pl.ds(blocks + source * slots, slots)] = landed[step]

    def rows_of(source):
        return pl.ds(pl.multiple_of(source * width, width), width)

    def full_copy(at, code, part):
        return pltpu.make_async_remote_copy(
            src_ref=hidden.at[at, part],
            dst_ref=gathered.at[part, rows_of(feat)],
            send_sem=full_send.at[at, part],
            recv_sem=full_recv.at[feat, part],
            device_id=(vert, dest_of(at, code)),
            device_id_type=MESH,
        )

    def aggregate_row(at, dest, part, row):
        picked = []
        line = dest * per_dest + part * group + row
        live = count[line]
        for place in range(depth):
            column = jnp.where(place < live, cols[place, line], dead)
            picked.append(extended[column])
        page = jnp.concatenate([pages[at, part, row, place] for place in range(depth)], axis=1)
        total = lax.dot_general(
            page,
            jnp.concatenate(picked, axis=1),
            (((1,), (1,)), ((), ())),
            preferred_element_type=jnp.float32,
        )
        return total.T.astype(jnp.bfloat16)

    def aggregate(at, code):
        towards = code % chips
        dest = dest_of(at, code)

        @pl.when((at % cores == 0) & (chip == 0) & (towards >= 2))
        def _():
            pl.semaphore_wait(above.at[towards], 1)

        @pl.when((at % cores == 0) & (chip == chips - 1) & (towards <= chips - 3))
        def _():
            pl.semaphore_wait(below.at[chips - 1 - towards], 1)

        for part in range(parts):
            page_copy(at, code, part).wait()
        for part in range(parts):
            for row in range(group):
                hidden[at, part, :, row * edge : (row + 1) * edge] = aggregate_row(
                    at, dest, part, row
                )
            full_copy(at, code, part).start()
        return next_code(at, code)

    code_end = lax.fori_loop(0, feats - 1, aggregate, code)
    for part in range(parts):
        page_copy(feats - 1, code_end, part).wait()
    for part in range(parts):
        for row in range(group):
            gathered[part, rows_of(feat), row * edge : (row + 1) * edge] = aggregate_row(
                feats - 1, feat, part, row
            )
    for table in tables[3:]:
        table.wait()

    def arrive(part):
        def one(step, carry):
            source = (feat + step) % feats
            pltpu.make_async_remote_copy(
                src_ref=hidden.at[0, part],
                dst_ref=gathered.at[part, rows_of(source)],
                send_sem=full_send.at[0, part],
                recv_sem=full_recv.at[source, part],
                device_id=(vert, source),
                device_id_type=MESH,
            ).wait_recv()
            return carry

        return one

    for part in range(parts):
        lax.fori_loop(1, feats, arrive(part), 0)
        mixed_rows = lax.dot_general(
            gathered[part], weight[...], (((0,), (0,)), ((), ())),
            preferred_element_type=jnp.float32,
        )
        out[part * span : (part + 1) * span, :] = jnp.maximum(
            mixed_rows + bias[...], jnp.float32(0.0)
        ).astype(jnp.bfloat16)

    def finish(at, code):
        for part in range(parts):
            full_copy(at, code, part).wait_send()
        return next_code(at, code)

    lax.fori_loop(0, feats - 1, finish, code)


def per_device(features, tiles, tile_cols, tile_count, send_list, weight, bias):
    blocks, depth, edge = tiles.shape[:3]
    width = features.shape[1]
    verts, feats = lax.axis_size("vert"), lax.axis_size("feat")
    cores = 2 if feats % 2 == 0 else 1
    slots = send_list.shape[2]
    per_dest = blocks // feats
    group = min(GROUP, per_dest)
    parts = per_dest // group
    rows = per_dest * edge
    dead = blocks + verts * slots
    chips = feats // cores
    dims = (verts, feats, cores, blocks, depth, edge, width, slots, group)
    held = [
        pltpu.VMEM((dead + 1, width, edge), jnp.bfloat16),
        pltpu.VMEM((width, blocks * edge), jnp.bfloat16),
        pltpu.VMEM((verts, slots, width, edge), jnp.bfloat16),
        pltpu.VMEM((verts, slots, width, edge), jnp.bfloat16),
        pltpu.VMEM((feats - 1, parts, width, group * edge), jnp.bfloat16),
        pltpu.VMEM((feats, parts, group, depth, edge, edge), jnp.bfloat16),
        pltpu.VMEM((parts, feats * width, group * edge), jnp.bfloat16),
    ]
    return pl.pallas_call(
        functools.partial(exchange_kernel, dims),
        out_shape=pltpu.VMEM((rows, weight.shape[1]), jnp.bfloat16),
        in_specs=[pl.BlockSpec(memory_space=pltpu.HBM)] * 7,
        out_specs=pl.BlockSpec(memory_space=pltpu.VMEM),
        scratch_shapes=[
            pltpu.SMEM((depth, blocks), jnp.int32),
            pltpu.SMEM((blocks,), jnp.int32),
            pltpu.SMEM(send_list.shape, jnp.int32),
            pltpu.SemaphoreType.DMA((5,)),
            *held,
            pltpu.VMEM(weight.shape, jnp.bfloat16),
            pltpu.VMEM(bias.shape, jnp.float32),
            pltpu.SemaphoreType.DMA,
            pltpu.SemaphoreType.DMA((feats, parts)),
            pltpu.SemaphoreType.DMA((verts,)),
            pltpu.SemaphoreType.DMA((verts,)),
            pltpu.SemaphoreType.DMA((feats - 1, parts)),
            pltpu.SemaphoreType.DMA((feats, parts)),
            pltpu.SemaphoreType.REGULAR((chips + 1,)),
            pltpu.SemaphoreType.REGULAR((chips + 1,)),
        ],
        compiler_params=pltpu.CompilerParams(
            collective_id=0, has_side_effects=True, vmem_limit_bytes=60 * 1024 * 1024
        ),
    )(*(pltpu.with_memory_space_constraint(one, pltpu.HBM) for one in (tile_cols.T, tile_count, send_list, features.T, tiles, weight, bias)))


def solution(mesh):
    return jax.shard_map(
        per_device,
        mesh=mesh,
        in_specs=(
            P("vert", "feat"),
            P("vert", None, None, None),
            P("vert", None),
            P("vert"),
            P("vert", None, None),
            P(),
            P(),
        ),
        out_specs=P(("vert", "feat"), None),
        check_vma=False,
    )
```

```python
import functools

import jax
import jax.numpy as jnp
from jax import lax
from jax.experimental import pallas as pl
from jax.experimental.pallas import tpu as pltpu
from jax.sharding import PartitionSpec as P

MESH = pl.DeviceIdType.MESH
GROUP = 4


def visiting_order(chip, chips):
    half = chips // 2
    low, high = list(range(half)), list(range(half, chips))
    if chip < half:
        return low[:chip][::-1] + high + low[chip + 1 :] + [chip]
    below, over = high[: chip - half], high[chip - half + 1 :]
    return low[:-1] + below + low[-1:] + over + [chip]


def order_code(chip, chips):
    codes = [
        sum(other * chips**at for at, other in enumerate(visiting_order(one, chips)))
        for one in range(chips)
    ]
    code = codes[0]
    for one in range(1, chips):
        code = jnp.where(chip == one, codes[one], code)
    return code


def exchange_kernel(
    dims, cols_in, count_in, send_in, features, tiles, weight_in, bias_in, out,
    cols, count, send, table_sem, extended, local, outgoing, landed, hidden, pages,
    gathered, weight, bias, load_sem, page_sem, halo_send, halo_recv, full_send, full_recv,
    above, below,
):
    verts, feats, cores, blocks, depth, edge, width, slots, group = dims
    chips = feats // cores
    per_dest = blocks // feats
    parts = per_dest // group
    span = group * edge
    dead = blocks + verts * slots
    vert = lax.axis_index("vert")
    feat = lax.axis_index("feat")
    chip, core = feat // cores, feat % cores

    def next_code(at, code):
        return jnp.where(at % cores == cores - 1, code // chips, code)

    def dest_of(at, code):
        mine = code % chips == chip
        return (code % chips) * cores + (core + at + jnp.where(mine, 1, 0)) % cores

    def page_copy(at, code, part):
        first = dest_of(at, code) * per_dest + part * group
        return pltpu.make_async_copy(
            tiles.at[pl.ds(first, group)], pages.at[at, part], page_sem.at[at, part]
        )

    local_copy = pltpu.make_async_copy(features, local, load_sem)
    local_copy.start()
    sources = (send_in, cols_in, count_in, weight_in, bias_in)
    tables = [
        pltpu.make_async_copy(source, target, table_sem.at[at])
        for at, (source, target) in enumerate(zip(sources, (send, cols, count, weight, bias)))
    ]
    for table in tables[:3]:
        table.start()
    barrier = pltpu.get_barrier_semaphore()
    for step in range(1, verts):
        pl.semaphore_signal(
            barrier, inc=1, device_id=((vert + step) % verts, feat), device_id_type=MESH
        )

    def greet(other):
        pl.semaphore_signal(barrier, inc=1, device_id=(vert, other), device_id_type=MESH)

    for step in range(1, cores):
        greet(chip * cores + (core + step) % cores)

    @pl.when(chip < chips - 1)
    def _():
        for other in range(cores):
            greet((chip + 1) * cores + other)

    code = order_code(chip, chips)
    walk = code
    for at in range(feats):
        for part in range(parts):
            page_copy(at, walk, part).start()
        walk = next_code(at, walk)
    for table in tables[3:]:
        table.start()
    extended[dead] = jnp.zeros((width, edge), jnp.bfloat16)
    tables[0].wait()
    local_copy.wait()
    for block in range(blocks):
        extended[block] = local[:, block * edge : (block + 1) * edge]
    for step in range(verts):
        peer = (vert + step) % verts
        for slot in range(slots):
            outgoing[step, slot] = extended[send[0, peer, slot]]
    pl.semaphore_wait(barrier, verts + cores - 2 + cores * jnp.where(chip > 0, 1, 0))

    def halo(step):
        return pltpu.make_async_remote_copy(
            src_ref=outgoing.at[step],
            dst_ref=landed.at[step],
            send_sem=halo_send.at[step],
            recv_sem=halo_recv.at[step],
            device_id=((vert + step) % verts, feat),
            device_id_type=MESH,
        )

    for peer in range(verts):

        @pl.when(peer != vert)
        def _():
            halo((peer + verts - vert) % verts).start()

    def tell(sem, other):
        pl.semaphore_signal(sem, inc=1, device_id=(vert, other), device_id_type=MESH)

    @pl.when(chip > 0)
    def _():
        tell(above.at[1], feat - cores)

    @pl.when(chip < chips - 1)
    def _():
        pl.semaphore_wait(above.at[1], 1)

    for far in range(2, chips):

        @pl.when((chip >= 1) & (chip + far - 1 <= chips - 1))
        def _():
            if far > 2:
                pl.semaphore_wait(above.at[far - 1], 1)
            tell(above.at[far], feat - cores)

        @pl.when((chip <= chips - 2) & (chip - far + 1 >= 0))
        def _():
            if far > 2:
                pl.semaphore_wait(below.at[far - 1], 1)
            tell(below.at[far], feat + cores)

    for table in tables[1:3]:
        table.wait()
    extended[pl.ds(blocks + vert * slots, slots)] = outgoing[0]
    for step in range(1, verts):
        halo(step).wait()
        source = (vert + verts - step) % verts
        extended[pl.ds(blocks + source * slots, slots)] = landed[step]

    def rows_of(source):
        return pl.ds(pl.multiple_of(source * width, width), width)

    def full_copy(at, code, part):
        return pltpu.make_async_remote_copy(
            src_ref=hidden.at[at, part],
            dst_ref=gathered.at[part, rows_of(feat)],
            send_sem=full_send.at[at, part],
            recv_sem=full_recv.at[feat, part],
            device_id=(vert, dest_of(at, code)),
            device_id_type=MESH,
        )

    def products(at, dest, part):
        totals = []
        for row in range(group):
            picked = []
            line = dest * per_dest + part * group + row
            live = count[line]
            for place in range(depth):
                column = jnp.where(place < live, cols[place, line], dead)
                picked.append(extended[column])
            page = jnp.concatenate([pages[at, part, row, place] for place in range(depth)], axis=1)
            totals.append(
                lax.dot_general(
                    page,
                    jnp.concatenate(picked, axis=1),
                    (((1,), (1,)), ((), ())),
                    preferred_element_type=jnp.float32,
                )
            )
        return totals

    def serve(first_at, code, sent):
        for away in range(cores):
            for part in range(parts):
                page_copy(first_at + away, code, part).wait()
        waiting = None

        def flush(at, part, totals, send_it):
            for row, total in enumerate(totals):
                block = total.T.astype(jnp.bfloat16)
                if send_it:
                    hidden[at, part, :, row * edge : (row + 1) * edge] = block
                else:
                    gathered[part, rows_of(feat), row * edge : (row + 1) * edge] = block
            if send_it:
                full_copy(at, code, part).start()

        for away in range(cores):
            at = first_at + away
            dest = dest_of(at, code)
            for part in range(parts):
                totals = products(at, dest, part)
                if waiting is not None:
                    flush(*waiting)
                waiting = (at, part, totals, away < sent)
        flush(*waiting)

    def serve_far(step, code):
        towards = code % chips

        @pl.when((chip == 0) & (towards >= 2))
        def _():
            pl.semaphore_wait(above.at[towards], 1)

        @pl.when((chip == chips - 1) & (towards <= chips - 3))
        def _():
            pl.semaphore_wait(below.at[chips - 1 - towards], 1)

        serve(step * cores, code, cores)
        return code // chips

    code_end = lax.fori_loop(0, chips - 1, serve_far, code)
    serve(feats - cores, code_end, cores - 1)
    for table in tables[3:]:
        table.wait()

    def arrive(part):
        def one(step, carry):
            source = (feat + step) % feats
            pltpu.make_async_remote_copy(
                src_ref=hidden.at[0, part],
                dst_ref=gathered.at[part, rows_of(source)],
                send_sem=full_send.at[0, part],
                recv_sem=full_recv.at[source, part],
                device_id=(vert, source),
                device_id_type=MESH,
            ).wait_recv()
            return carry

        return one

    for part in range(parts):
        lax.fori_loop(1, feats, arrive(part), 0)
        mixed_rows = lax.dot_general(
            gathered[part], weight[...], (((0,), (0,)), ((), ())),
            preferred_element_type=jnp.float32,
        )
        out[part * span : (part + 1) * span, :] = jnp.maximum(
            mixed_rows + bias[...], jnp.float32(0.0)
        ).astype(jnp.bfloat16)

    def finish(at, code):
        for part in range(parts):
            full_copy(at, code, part).wait_send()
        return next_code(at, code)

    lax.fori_loop(0, feats - 1, finish, code)


def per_device(features, tiles, tile_cols, tile_count, send_list, weight, bias):
    blocks, depth, edge = tiles.shape[:3]
    width = features.shape[1]
    verts, feats = lax.axis_size("vert"), lax.axis_size("feat")
    cores = 2 if feats % 2 == 0 else 1
    slots = send_list.shape[2]
    per_dest = blocks // feats
    group = min(GROUP, per_dest)
    parts = per_dest // group
    rows = per_dest * edge
    dead = blocks + verts * slots
    chips = feats // cores
    dims = (verts, feats, cores, blocks, depth, edge, width, slots, group)
    held = [
        pltpu.VMEM((dead + 1, width, edge), jnp.bfloat16),
        pltpu.VMEM((width, blocks * edge), jnp.bfloat16),
        pltpu.VMEM((verts, slots, width, edge), jnp.bfloat16),
        pltpu.VMEM((verts, slots, width, edge), jnp.bfloat16),
        pltpu.VMEM((feats - 1, parts, width, group * edge), jnp.bfloat16),
        pltpu.VMEM((feats, parts, group, depth, edge, edge), jnp.bfloat16),
        pltpu.VMEM((parts, feats * width, group * edge), jnp.bfloat16),
    ]
    return pl.pallas_call(
        functools.partial(exchange_kernel, dims),
        out_shape=pltpu.VMEM((rows, weight.shape[1]), jnp.bfloat16),
        in_specs=[pl.BlockSpec(memory_space=pltpu.HBM)] * 7,
        out_specs=pl.BlockSpec(memory_space=pltpu.VMEM),
        scratch_shapes=[
            pltpu.SMEM((depth, blocks), jnp.int32),
            pltpu.SMEM((blocks,), jnp.int32),
            pltpu.SMEM(send_list.shape, jnp.int32),
            pltpu.SemaphoreType.DMA((5,)),
            *held,
            pltpu.VMEM(weight.shape, jnp.bfloat16),
            pltpu.VMEM(bias.shape, jnp.float32),
            pltpu.SemaphoreType.DMA,
            pltpu.SemaphoreType.DMA((feats, parts)),
            pltpu.SemaphoreType.DMA((verts,)),
            pltpu.SemaphoreType.DMA((verts,)),
            pltpu.SemaphoreType.DMA((feats - 1, parts)),
            pltpu.SemaphoreType.DMA((feats, parts)),
            pltpu.SemaphoreType.REGULAR((chips + 1,)),
            pltpu.SemaphoreType.REGULAR((chips + 1,)),
        ],
        compiler_params=pltpu.CompilerParams(
            collective_id=0, has_side_effects=True, vmem_limit_bytes=60 * 1024 * 1024
        ),
    )(*(pltpu.with_memory_space_constraint(one, pltpu.HBM) for one in (tile_cols.T, tile_count, send_list, features.T, tiles, weight, bias)))


def solution(mesh):
    return jax.shard_map(
        per_device,
        mesh=mesh,
        in_specs=(
            P("vert", "feat"),
            P("vert", None, None, None),
            P("vert", None),
            P("vert"),
            P("vert", None, None),
            P(),
            P(),
        ),
        out_specs=P(("vert", "feat"), None),
        check_vma=False,
    )
```

```python
import functools

import jax
import jax.numpy as jnp
from jax import lax
from jax.experimental import pallas as pl
from jax.experimental.pallas import tpu as pltpu
from jax.sharding import PartitionSpec as P

MESH = pl.DeviceIdType.MESH
GROUP = 4
FINE = 2
SWAP = (2, 3)


def visiting_order(chip, chips):
    half = chips // 2
    low, high = list(range(half)), list(range(half, chips))
    if chip < half:
        return low[:chip][::-1] + high + low[chip + 1 :] + [chip]
    below, over = high[: chip - half], high[chip - half + 1 :]
    return low[:-1] + below + low[-1:] + over + [chip]


def order_code(chip, chips):
    codes = [
        sum(other * chips**at for at, other in enumerate(visiting_order(one, chips)))
        for one in range(chips)
    ]
    code = codes[0]
    for one in range(1, chips):
        code = jnp.where(chip == one, codes[one], code)
    return code


def exchange_kernel(
    dims, cols_in, count_in, send_in, features, tiles, weight_in, bias_in, out,
    cols, count, send, table_sem, extended, local, outgoing, landed, hidden, pages,
    gathered, weight, bias, load_sem, page_sem, halo_send, halo_recv, full_send, full_recv,
    above, below,
):
    verts, feats, cores, blocks, depth, edge, width, slots, group = dims
    chips = feats // cores
    per_dest = blocks // feats
    parts = per_dest // group
    span = group * edge
    dead = blocks + verts * slots
    vert = lax.axis_index("vert")
    feat = lax.axis_index("feat")
    chip, core = feat // cores, feat % cores

    def next_code(at, code):
        return jnp.where(at % cores == cores - 1, code // chips, code)

    def dest_of(at, code):
        mine = code % chips == chip
        return (code % chips) * cores + (core + at + jnp.where(mine, 1, 0)) % cores

    def page_copy(at, code, part):
        first = dest_of(at, code) * per_dest + part * group
        return pltpu.make_async_copy(
            tiles.at[pl.ds(first, group)], pages.at[at, part], page_sem.at[at, part]
        )

    local_copy = pltpu.make_async_copy(features, local, load_sem)
    local_copy.start()
    sources = (send_in, cols_in, count_in, weight_in, bias_in)
    tables = [
        pltpu.make_async_copy(source, target, table_sem.at[at])
        for at, (source, target) in enumerate(zip(sources, (send, cols, count, weight, bias)))
    ]
    for table in tables[:3]:
        table.start()
    barrier = pltpu.get_barrier_semaphore()
    for step in range(1, verts):
        pl.semaphore_signal(
            barrier, inc=1, device_id=((vert + step) % verts, feat), device_id_type=MESH
        )

    def greet(other):
        pl.semaphore_signal(barrier, inc=1, device_id=(vert, other), device_id_type=MESH)

    for step in range(1, cores):
        greet(chip * cores + (core + step) % cores)

    @pl.when(chip < chips - 1)
    def _():
        for other in range(cores):
            greet((chip + 1) * cores + other)

    code = order_code(chip, chips)
    walk = code
    for at in range(feats):
        for part in range(parts):
            page_copy(at, walk, part).start()
        walk = next_code(at, walk)
    for table in tables[3:]:
        table.start()
    extended[dead] = jnp.zeros((width, edge), jnp.bfloat16)
    tables[0].wait()
    local_copy.wait()
    for block in range(blocks):
        extended[block] = local[:, block * edge : (block + 1) * edge]
    for step in range(verts):
        peer = (vert + step) % verts
        for slot in range(slots):
            outgoing[step, slot] = extended[send[0, peer, slot]]
    pl.semaphore_wait(barrier, verts + cores - 2 + cores * jnp.where(chip > 0, 1, 0))

    def halo(step):
        return pltpu.make_async_remote_copy(
            src_ref=outgoing.at[step],
            dst_ref=landed.at[step],
            send_sem=halo_send.at[step],
            recv_sem=halo_recv.at[step],
            device_id=((vert + step) % verts, feat),
            device_id_type=MESH,
        )

    for peer in range(verts):

        @pl.when(peer != vert)
        def _():
            halo((peer + verts - vert) % verts).start()

    def tell(sem, other):
        pl.semaphore_signal(sem, inc=1, device_id=(vert, other), device_id_type=MESH)

    @pl.when(chip > 0)
    def _():
        tell(above.at[1], feat - cores)

    @pl.when(chip < chips - 1)
    def _():
        pl.semaphore_wait(above.at[1], 1)

    for far in range(2, chips):

        @pl.when((chip >= 1) & (chip + far - 1 <= chips - 1))
        def _():
            if far > 2:
                pl.semaphore_wait(above.at[far - 1], 1)
            tell(above.at[far], feat - cores)

        @pl.when((chip <= chips - 2) & (chip - far + 1 >= 0))
        def _():
            if far > 2:
                pl.semaphore_wait(below.at[far - 1], 1)
            tell(below.at[far], feat + cores)

    for table in tables[1:3]:
        table.wait()
    extended[pl.ds(blocks + vert * slots, slots)] = outgoing[0]
    for step in range(1, verts):
        halo(step).wait()
        source = (vert + verts - step) % verts
        extended[pl.ds(blocks + source * slots, slots)] = landed[step]

    def rows_of(source):
        return pl.ds(pl.multiple_of(source * width, width), width)

    def full_copy(at, code, part, rows):
        columns = pl.ds(rows[0] * edge, len(rows) * edge)
        return pltpu.make_async_remote_copy(
            src_ref=hidden.at[at, part, :, columns],
            dst_ref=gathered.at[part, rows_of(feat), columns],
            send_sem=full_send.at[at, part],
            recv_sem=full_recv.at[feat, part],
            device_id=(vert, dest_of(at, code)),
            device_id_type=MESH,
        )

    def products(at, dest, part, rows):
        totals = []
        for row in rows:
            picked = []
            line = dest * per_dest + part * group + row
            live = count[line]
            for place in range(depth):
                column = jnp.where(place < live, cols[place, line], dead)
                picked.append(extended[column])
            page = jnp.concatenate([pages[at, part, row, place] for place in range(depth)], axis=1)
            vectors = jnp.concatenate(picked, axis=1)
            both = (((1,), (1,)), ((), ()))
            if row in SWAP:
                total = lax.dot_general(vectors, page, both, preferred_element_type=jnp.float32)
            else:
                total = lax.dot_general(page, vectors, both, preferred_element_type=jnp.float32).T
            totals.append(total)
        return totals

    def serve(first_at, code, sent, fine=1):
        for away in range(cores):
            for part in range(parts):
                page_copy(first_at + away, code, part).wait()
        waiting = None

        def flush(at, part, rows, totals, send_it):
            for row, total in zip(rows, totals):
                block = total.astype(jnp.bfloat16)
                if send_it:
                    hidden[at, part, :, row * edge : (row + 1) * edge] = block
                else:
                    gathered[part, rows_of(feat), row * edge : (row + 1) * edge] = block
            if send_it:
                full_copy(at, code, part, rows).start()

        for away in range(cores):
            at = first_at + away
            dest = dest_of(at, code)
            for part in range(parts):
                pieces = fine if away == 0 and part == 0 else 1
                for piece in range(pieces):
                    rows = range(group * piece // pieces, group * (piece + 1) // pieces)
                    totals = products(at, dest, part, rows)
                    if waiting is not None:
                        flush(*waiting)
                    waiting = (at, part, rows, totals, away < sent)
        flush(*waiting)

    def serve_far(step, code):
        towards = code % chips

        @pl.when((chip == 0) & (towards >= 2))
        def _():
            pl.semaphore_wait(above.at[towards], 1)

        @pl.when((chip == chips - 1) & (towards <= chips - 3))
        def _():
            pl.semaphore_wait(below.at[chips - 1 - towards], 1)

        serve(step * cores, code, cores, FINE if isinstance(step, int) else 1)
        return code // chips

    code_end = code
    if chips > 1:
        code_end = lax.fori_loop(1, chips - 1, serve_far, serve_far(0, code))
    serve(feats - cores, code_end, cores - 1)
    for table in tables[3:]:
        table.wait()

    def arrive(part):
        def one(step, carry):
            source = (feat + step) % feats
            pltpu.make_async_remote_copy(
                src_ref=hidden.at[0, part],
                dst_ref=gathered.at[part, rows_of(source)],
                send_sem=full_send.at[0, part],
                recv_sem=full_recv.at[source, part],
                device_id=(vert, source),
                device_id_type=MESH,
            ).wait_recv()
            return carry

        return one

    for part in range(parts):
        lax.fori_loop(1, feats, arrive(part), 0)
        mixed_rows = lax.dot_general(
            gathered[part], weight[...], (((0,), (0,)), ((), ())),
            preferred_element_type=jnp.float32,
        )
        out[part * span : (part + 1) * span, :] = jnp.maximum(
            mixed_rows + bias[...], jnp.float32(0.0)
        ).astype(jnp.bfloat16)

    def finish(at, code):
        for part in range(parts):
            full_copy(at, code, part, range(group)).wait_send()
        return next_code(at, code)

    lax.fori_loop(0, feats - 1, finish, code)


def per_device(features, tiles, tile_cols, tile_count, send_list, weight, bias):
    blocks, depth, edge = tiles.shape[:3]
    width = features.shape[1]
    verts, feats = lax.axis_size("vert"), lax.axis_size("feat")
    cores = 2 if feats % 2 == 0 else 1
    slots = send_list.shape[2]
    per_dest = blocks // feats
    group = min(GROUP, per_dest)
    parts = per_dest // group
    rows = per_dest * edge
    dead = blocks + verts * slots
    chips = feats // cores
    dims = (verts, feats, cores, blocks, depth, edge, width, slots, group)
    held = [
        pltpu.VMEM((dead + 1, width, edge), jnp.bfloat16),
        pltpu.VMEM((width, blocks * edge), jnp.bfloat16),
        pltpu.VMEM((verts, slots, width, edge), jnp.bfloat16),
        pltpu.VMEM((verts, slots, width, edge), jnp.bfloat16),
        pltpu.VMEM((feats - 1, parts, width, group * edge), jnp.bfloat16),
        pltpu.VMEM((feats, parts, group, depth, edge, edge), jnp.bfloat16),
        pltpu.VMEM((parts, feats * width, group * edge), jnp.bfloat16),
    ]
    return pl.pallas_call(
        functools.partial(exchange_kernel, dims),
        out_shape=pltpu.VMEM((rows, weight.shape[1]), jnp.bfloat16),
        in_specs=[pl.BlockSpec(memory_space=pltpu.HBM)] * 7,
        out_specs=pl.BlockSpec(memory_space=pltpu.VMEM),
        scratch_shapes=[
            pltpu.SMEM((depth, blocks), jnp.int32),
            pltpu.SMEM((blocks,), jnp.int32),
            pltpu.SMEM(send_list.shape, jnp.int32),
            pltpu.SemaphoreType.DMA((5,)),
            *held,
            pltpu.VMEM(weight.shape, jnp.bfloat16),
            pltpu.VMEM(bias.shape, jnp.float32),
            pltpu.SemaphoreType.DMA,
            pltpu.SemaphoreType.DMA((feats, parts)),
            pltpu.SemaphoreType.DMA((verts,)),
            pltpu.SemaphoreType.DMA((verts,)),
            pltpu.SemaphoreType.DMA((feats - 1, parts)),
            pltpu.SemaphoreType.DMA((feats, parts)),
            pltpu.SemaphoreType.REGULAR((chips + 1,)),
            pltpu.SemaphoreType.REGULAR((chips + 1,)),
        ],
        compiler_params=pltpu.CompilerParams(
            collective_id=0, has_side_effects=True, vmem_limit_bytes=60 * 1024 * 1024
        ),
    )(*(pltpu.with_memory_space_constraint(one, pltpu.HBM) for one in (tile_cols.T, tile_count, send_list, features.T, tiles, weight, bias)))


def solution(mesh):
    return jax.shard_map(
        per_device,
        mesh=mesh,
        in_specs=(
            P("vert", "feat"),
            P("vert", None, None, None),
            P("vert", None),
            P("vert"),
            P("vert", None, None),
            P(),
            P(),
        ),
        out_specs=P(("vert", "feat"), None),
        check_vma=False,
    )
```

```python
import functools

import jax
import jax.numpy as jnp
from jax import lax
from jax.experimental import pallas as pl
from jax.experimental.pallas import tpu as pltpu
from jax.sharding import PartitionSpec as P

MESH = pl.DeviceIdType.MESH
GROUP = 4
SWAP = (1,)


def visiting_order(chip, chips):
    half = chips // 2
    low, high = list(range(half)), list(range(half, chips))
    if chip < half:
        return low[:chip][::-1] + high + low[chip + 1 :] + [chip]
    below, over = high[: chip - half], high[chip - half + 1 :]
    return low[:-1] + below + low[-1:] + over + [chip]


def order_code(chip, chips):
    codes = [
        sum(other * chips**at for at, other in enumerate(visiting_order(one, chips)))
        for one in range(chips)
    ]
    code = codes[0]
    for one in range(1, chips):
        code = jnp.where(chip == one, codes[one], code)
    return code


def exchange_kernel(
    dims, cols_in, count_in, send_in, features, tiles, weight_in, bias_in, out,
    cols, count, send, table_sem, extended, local, outgoing, landed, hidden, pages,
    gathered, weight, bias, load_sem, page_sem, halo_send, halo_recv, full_send, full_recv,
    above, below,
):
    verts, feats, cores, blocks, depth, edge, width, slots, group = dims
    chips = feats // cores
    per_dest = blocks // feats
    parts = per_dest // group
    span = group * edge
    dead = blocks + verts * slots
    vert = lax.axis_index("vert")
    feat = lax.axis_index("feat")
    chip, core = feat // cores, feat % cores

    def next_code(at, code):
        return jnp.where(at % cores == cores - 1, code // chips, code)

    def dest_of(at, code):
        mine = code % chips == chip
        return (code % chips) * cores + (core + at + jnp.where(mine, 1, 0)) % cores

    def page_copy(at, code, part):
        first = dest_of(at, code) * per_dest + part * group
        return pltpu.make_async_copy(
            tiles.at[pl.ds(first, group)], pages.at[at, part], page_sem.at[at, part]
        )

    local_copy = pltpu.make_async_copy(features, local, load_sem)
    local_copy.start()
    sources = (send_in, cols_in, count_in, weight_in, bias_in)
    tables = [
        pltpu.make_async_copy(source, target, table_sem.at[at])
        for at, (source, target) in enumerate(zip(sources, (send, cols, count, weight, bias)))
    ]
    for table in tables[:3]:
        table.start()
    barrier = pltpu.get_barrier_semaphore()
    for step in range(1, verts):
        pl.semaphore_signal(
            barrier, inc=1, device_id=((vert + step) % verts, feat), device_id_type=MESH
        )

    def greet(other):
        pl.semaphore_signal(barrier, inc=1, device_id=(vert, other), device_id_type=MESH)

    for step in range(1, cores):
        greet(chip * cores + (core + step) % cores)

    @pl.when(chip < chips - 1)
    def _():
        for other in range(cores):
            greet((chip + 1) * cores + other)

    code = order_code(chip, chips)
    walk = code
    for at in range(feats):
        for part in range(parts):
            page_copy(at, walk, part).start()
        walk = next_code(at, walk)
    for table in tables[3:]:
        table.start()
    extended[dead] = jnp.zeros((width, edge), jnp.bfloat16)
    tables[0].wait()
    local_copy.wait()
    for block in range(blocks):
        extended[block] = local[:, block * edge : (block + 1) * edge]
    for step in range(verts):
        peer = (vert + step) % verts
        for slot in range(slots):
            outgoing[step, slot] = extended[send[0, peer, slot]]
    pl.semaphore_wait(barrier, verts + cores - 2 + cores * jnp.where(chip > 0, 1, 0))

    def halo(step):
        return pltpu.make_async_remote_copy(
            src_ref=outgoing.at[step],
            dst_ref=landed.at[step],
            send_sem=halo_send.at[step],
            recv_sem=halo_recv.at[step],
            device_id=((vert + step) % verts, feat),
            device_id_type=MESH,
        )

    for peer in range(verts):

        @pl.when(peer != vert)
        def _():
            halo((peer + verts - vert) % verts).start()

    def tell(sem, other):
        pl.semaphore_signal(sem, inc=1, device_id=(vert, other), device_id_type=MESH)

    @pl.when(chip > 0)
    def _():
        tell(above.at[1], feat - cores)

    @pl.when(chip < chips - 1)
    def _():
        pl.semaphore_wait(above.at[1], 1)

    for far in range(2, chips):

        @pl.when((chip >= 1) & (chip + far - 1 <= chips - 1))
        def _():
            if far > 2:
                pl.semaphore_wait(above.at[far - 1], 1)
            tell(above.at[far], feat - cores)

        @pl.when((chip <= chips - 2) & (chip - far + 1 >= 0))
        def _():
            if far > 2:
                pl.semaphore_wait(below.at[far - 1], 1)
            tell(below.at[far], feat + cores)

    for table in tables[1:3]:
        table.wait()
    extended[pl.ds(blocks + vert * slots, slots)] = outgoing[0]
    for step in range(1, verts):
        halo(step).wait()
        source = (vert + verts - step) % verts
        extended[pl.ds(blocks + source * slots, slots)] = landed[step]

    def rows_of(source):
        return pl.ds(pl.multiple_of(source * width, width), width)

    def full_copy(at, code, first, rows):
        columns = pl.ds(first * edge, rows * edge)
        return pltpu.make_async_remote_copy(
            src_ref=hidden.at[at, :, columns],
            dst_ref=gathered.at[rows_of(feat), columns],
            send_sem=full_send.at[at],
            recv_sem=full_recv.at[feat],
            device_id=(vert, dest_of(at, code)),
            device_id_type=MESH,
        )

    def products(at, dest, part, rows):
        totals = []
        for row in rows:
            picked = []
            line = dest * per_dest + part * group + row
            live = count[line]
            for place in range(depth):
                column = jnp.where(place < live, cols[place, line], dead)
                picked.append(extended[column])
            page = jnp.concatenate([pages[at, part, row, place] for place in range(depth)], axis=1)
            vectors = jnp.concatenate(picked, axis=1)
            both = (((1,), (1,)), ((), ()))
            if row in SWAP:
                total = lax.dot_general(vectors, page, both, preferred_element_type=jnp.float32)
            else:
                total = lax.dot_general(page, vectors, both, preferred_element_type=jnp.float32).T
            totals.append(total)
        return totals

    def serve(first_at, code, sent, early):
        for away in range(cores):
            for part in range(parts):
                page_copy(first_at + away, code, part).wait()
        waiting = None

        def flush(at, first, totals, send_it):
            for row, total in enumerate(totals):
                block = total.astype(jnp.bfloat16)
                columns = slice((first + row) * edge, (first + row + 1) * edge)
                if send_it:
                    hidden[at, :, columns] = block
                else:
                    gathered[rows_of(feat), columns] = block
            done = first + len(totals)
            if send_it and early:
                full_copy(at, code, first, len(totals)).start()
            elif send_it and done == per_dest:
                full_copy(at, code, 0, per_dest).start()

        for away in range(cores):
            at = first_at + away
            dest = dest_of(at, code)
            for part in range(parts):
                totals = products(at, dest, part, range(group))
                if waiting is not None:
                    flush(*waiting)
                waiting = (at, part * group, totals, away < sent)
        flush(*waiting)

    def serve_far(step, code):
        towards = code % chips

        @pl.when((chip == 0) & (towards >= 2))
        def _():
            pl.semaphore_wait(above.at[towards], 1)

        @pl.when((chip == chips - 1) & (towards <= chips - 3))
        def _():
            pl.semaphore_wait(below.at[chips - 1 - towards], 1)

        serve(step * cores, code, cores, isinstance(step, int))
        return code // chips

    code_end = code
    if chips > 1:
        code_end = lax.fori_loop(1, chips - 1, serve_far, serve_far(0, code))
    serve(feats - cores, code_end, cores - 1, False)
    for table in tables[3:]:
        table.wait()

    def arrive(step, carry):
        source = (feat + step) % feats
        pltpu.make_async_remote_copy(
            src_ref=hidden.at[0],
            dst_ref=gathered.at[rows_of(source)],
            send_sem=full_send.at[0],
            recv_sem=full_recv.at[source],
            device_id=(vert, source),
            device_id_type=MESH,
        ).wait_recv()
        return carry

    lax.fori_loop(1, feats, arrive, 0)
    for part in range(parts):
        columns = slice(part * span, (part + 1) * span)
        mixed_rows = lax.dot_general(
            gathered[:, columns], weight[...], (((0,), (0,)), ((), ())),
            preferred_element_type=jnp.float32,
        )
        out[columns, :] = jnp.maximum(mixed_rows + bias[...], jnp.float32(0.0)).astype(
            jnp.bfloat16
        )

    def finish(at, code):
        full_copy(at, code, 0, per_dest).wait_send()
        return next_code(at, code)

    lax.fori_loop(0, feats - 1, finish, code)


def per_device(features, tiles, tile_cols, tile_count, send_list, weight, bias):
    blocks, depth, edge = tiles.shape[:3]
    width = features.shape[1]
    verts, feats = lax.axis_size("vert"), lax.axis_size("feat")
    cores = 2 if feats % 2 == 0 else 1
    slots = send_list.shape[2]
    per_dest = blocks // feats
    group = min(GROUP, per_dest)
    parts = per_dest // group
    rows = per_dest * edge
    dead = blocks + verts * slots
    chips = feats // cores
    dims = (verts, feats, cores, blocks, depth, edge, width, slots, group)
    held = [
        pltpu.VMEM((dead + 1, width, edge), jnp.bfloat16),
        pltpu.VMEM((width, blocks * edge), jnp.bfloat16),
        pltpu.VMEM((verts, slots, width, edge), jnp.bfloat16),
        pltpu.VMEM((verts, slots, width, edge), jnp.bfloat16),
        pltpu.VMEM((feats - 1, width, rows), jnp.bfloat16),
        pltpu.VMEM((feats, parts, group, depth, edge, edge), jnp.bfloat16),
        pltpu.VMEM((feats * width, rows), jnp.bfloat16),
    ]
    return pl.pallas_call(
        functools.partial(exchange_kernel, dims),
        out_shape=pltpu.VMEM((rows, weight.shape[1]), jnp.bfloat16),
        in_specs=[pl.BlockSpec(memory_space=pltpu.HBM)] * 7,
        out_specs=pl.BlockSpec(memory_space=pltpu.VMEM),
        scratch_shapes=[
            pltpu.SMEM((depth, blocks), jnp.int32),
            pltpu.SMEM((blocks,), jnp.int32),
            pltpu.SMEM(send_list.shape, jnp.int32),
            pltpu.SemaphoreType.DMA((5,)),
            *held,
            pltpu.VMEM(weight.shape, jnp.bfloat16),
            pltpu.VMEM(bias.shape, jnp.float32),
            pltpu.SemaphoreType.DMA,
            pltpu.SemaphoreType.DMA((feats, parts)),
            pltpu.SemaphoreType.DMA((verts,)),
            pltpu.SemaphoreType.DMA((verts,)),
            pltpu.SemaphoreType.DMA((feats - 1,)),
            pltpu.SemaphoreType.DMA((feats,)),
            pltpu.SemaphoreType.REGULAR((chips + 1,)),
            pltpu.SemaphoreType.REGULAR((chips + 1,)),
        ],
        compiler_params=pltpu.CompilerParams(
            collective_id=0, has_side_effects=True, vmem_limit_bytes=60 * 1024 * 1024
        ),
    )(*(pltpu.with_memory_space_constraint(one, pltpu.HBM) for one in (tile_cols.T, tile_count, send_list, features.T, tiles, weight, bias)))


def solution(mesh):
    return jax.shard_map(
        per_device,
        mesh=mesh,
        in_specs=(
            P("vert", "feat"),
            P("vert", None, None, None),
            P("vert", None),
            P("vert"),
            P("vert", None, None),
            P(),
            P(),
        ),
        out_specs=P(("vert", "feat"), None),
        check_vma=False,
    )
```

```python
import functools

import jax
import jax.numpy as jnp
from jax import lax
from jax.experimental import pallas as pl
from jax.experimental.pallas import tpu as pltpu
from jax.sharding import PartitionSpec as P

MESH = pl.DeviceIdType.MESH
GROUP = 4
SWAP = (1,)


def visiting_order(chip, chips):
    half = chips // 2
    low, high = list(range(half)), list(range(half, chips))
    if chip < half:
        return low[:chip][::-1] + high + low[chip + 1 :] + [chip]
    below, over = high[: chip - half], high[chip - half + 1 :]
    return low[:-1] + below + over + low[-1:] + [chip]


def order_code(chip, chips):
    codes = [
        sum(other * chips**at for at, other in enumerate(visiting_order(one, chips)))
        for one in range(chips)
    ]
    code = codes[0]
    for one in range(1, chips):
        code = jnp.where(chip == one, codes[one], code)
    return code


def exchange_kernel(
    dims, cols_in, count_in, send_in, features, tiles, weight_in, bias_in, out,
    cols, count, send, table_sem, extended, local, outgoing, landed, hidden, pages,
    gathered, weight, bias, load_sem, page_sem, halo_send, halo_recv, full_send, full_recv,
    above, below,
):
    verts, feats, cores, blocks, depth, edge, width, slots, group = dims
    chips = feats // cores
    per_dest = blocks // feats
    parts = per_dest // group
    span = group * edge
    dead = blocks + verts * slots
    vert = lax.axis_index("vert")
    feat = lax.axis_index("feat")
    chip, core = feat // cores, feat % cores

    def next_code(at, code):
        return jnp.where(at % cores == cores - 1, code // chips, code)

    def dest_of(at, code):
        mine = code % chips == chip
        return (code % chips) * cores + (core + at + jnp.where(mine, 1, 0)) % cores

    def page_copy(at, code, part):
        first = dest_of(at, code) * per_dest + part * group
        return pltpu.make_async_copy(
            tiles.at[pl.ds(first, group)], pages.at[at, part], page_sem.at[at, part]
        )

    local_copy = pltpu.make_async_copy(features, local, load_sem)
    local_copy.start()
    sources = (send_in, cols_in, count_in, weight_in, bias_in)
    tables = [
        pltpu.make_async_copy(source, target, table_sem.at[at])
        for at, (source, target) in enumerate(zip(sources, (send, cols, count, weight, bias)))
    ]
    for table in tables[:3]:
        table.start()
    barrier = pltpu.get_barrier_semaphore()
    for step in range(1, verts):
        pl.semaphore_signal(
            barrier, inc=1, device_id=((vert + step) % verts, feat), device_id_type=MESH
        )

    def greet(other):
        pl.semaphore_signal(barrier, inc=1, device_id=(vert, other), device_id_type=MESH)

    for step in range(1, cores):
        greet(chip * cores + (core + step) % cores)

    @pl.when(chip < chips - 1)
    def _():
        for other in range(cores):
            greet((chip + 1) * cores + other)

    code = order_code(chip, chips)
    walk = code
    for at in range(feats):
        for part in range(parts):
            page_copy(at, walk, part).start()
        walk = next_code(at, walk)
    for table in tables[3:]:
        table.start()
    extended[dead] = jnp.zeros((width, edge), jnp.bfloat16)
    tables[0].wait()
    local_copy.wait()
    for block in range(blocks):
        extended[block] = local[:, block * edge : (block + 1) * edge]
    for step in range(verts):
        peer = (vert + step) % verts
        for slot in range(slots):
            outgoing[step, slot] = extended[send[0, peer, slot]]
    pl.semaphore_wait(barrier, verts + cores - 2 + cores * jnp.where(chip > 0, 1, 0))

    def halo(step):
        return pltpu.make_async_remote_copy(
            src_ref=outgoing.at[step],
            dst_ref=landed.at[step],
            send_sem=halo_send.at[step],
            recv_sem=halo_recv.at[step],
            device_id=((vert + step) % verts, feat),
            device_id_type=MESH,
        )

    for peer in range(verts):

        @pl.when(peer != vert)
        def _():
            halo((peer + verts - vert) % verts).start()

    def tell(sem, other):
        pl.semaphore_signal(sem, inc=1, device_id=(vert, other), device_id_type=MESH)

    @pl.when(chip > 0)
    def _():
        tell(above.at[1], feat - cores)

    @pl.when(chip < chips - 1)
    def _():
        pl.semaphore_wait(above.at[1], 1)

    for far in range(2, chips):

        @pl.when((chip >= 1) & (chip + far - 1 <= chips - 1))
        def _():
            if far > 2:
                pl.semaphore_wait(above.at[far - 1], 1)
            tell(above.at[far], feat - cores)

        @pl.when((chip <= chips - 2) & (chip - far + 1 >= 0))
        def _():
            if far > 2:
                pl.semaphore_wait(below.at[far - 1], 1)
            tell(below.at[far], feat + cores)

    for table in tables[1:3]:
        table.wait()
    extended[pl.ds(blocks + vert * slots, slots)] = outgoing[0]
    for step in range(1, verts):
        halo(step).wait()
        source = (vert + verts - step) % verts
        extended[pl.ds(blocks + source * slots, slots)] = landed[step]

    def rows_of(source):
        return pl.ds(pl.multiple_of(source * width, width), width)

    def full_copy(at, code, first, rows):
        columns = pl.ds(first * edge, rows * edge)
        return pltpu.make_async_remote_copy(
            src_ref=hidden.at[at, :, columns],
            dst_ref=gathered.at[rows_of(feat), columns],
            send_sem=full_send.at[at],
            recv_sem=full_recv.at[feat],
            device_id=(vert, dest_of(at, code)),
            device_id_type=MESH,
        )

    def products(at, dest, part, rows):
        totals = []
        for row in rows:
            picked = []
            line = dest * per_dest + part * group + row
            live = count[line]
            for place in range(depth):
                column = jnp.where(place < live, cols[place, line], dead)
                picked.append(extended[column])
            page = jnp.concatenate([pages[at, part, row, place] for place in range(depth)], axis=1)
            vectors = jnp.concatenate(picked, axis=1)
            both = (((1,), (1,)), ((), ()))
            if row in SWAP:
                total = lax.dot_general(vectors, page, both, preferred_element_type=jnp.float32)
            else:
                total = lax.dot_general(page, vectors, both, preferred_element_type=jnp.float32).T
            totals.append(total)
        return totals

    def serve(first_at, code, sent, early):
        for away in range(cores):
            for part in range(parts):
                page_copy(first_at + away, code, part).wait()
        waiting = None

        def flush(at, first, totals, send_it):
            for row, total in enumerate(totals):
                block = total.astype(jnp.bfloat16)
                columns = slice((first + row) * edge, (first + row + 1) * edge)
                if send_it:
                    hidden[at, :, columns] = block
                else:
                    gathered[rows_of(feat), columns] = block
            done = first + len(totals)
            if send_it and early:
                full_copy(at, code, first, len(totals)).start()
            elif send_it and done == per_dest:
                full_copy(at, code, 0, per_dest).start()

        for away in range(cores):
            at = first_at + away
            dest = dest_of(at, code)
            for part in range(parts):
                totals = products(at, dest, part, range(group))
                if waiting is not None:
                    flush(*waiting)
                waiting = (at, part * group, totals, away < sent)
        flush(*waiting)

    def serve_far(step, code):
        towards = code % chips

        @pl.when((chip == 0) & (towards >= 2))
        def _():
            pl.semaphore_wait(above.at[towards], 1)

        @pl.when((chip == chips - 1) & (towards <= chips - 3))
        def _():
            pl.semaphore_wait(below.at[chips - 1 - towards], 1)

        serve(step * cores, code, cores, isinstance(step, int))
        return code // chips

    code_end = code
    if chips > 1:
        code_end = lax.fori_loop(1, chips - 1, serve_far, serve_far(0, code))
    serve(feats - cores, code_end, cores - 1, False)
    for table in tables[3:]:
        table.wait()

    def arrive(step, carry):
        source = (feat + step) % feats
        pltpu.make_async_remote_copy(
            src_ref=hidden.at[0],
            dst_ref=gathered.at[rows_of(source)],
            send_sem=full_send.at[0],
            recv_sem=full_recv.at[source],
            device_id=(vert, source),
            device_id_type=MESH,
        ).wait_recv()
        return carry

    lax.fori_loop(1, feats, arrive, 0)
    for part in range(parts):
        columns = slice(part * span, (part + 1) * span)
        mixed_rows = lax.dot_general(
            gathered[:, columns], weight[...], (((0,), (0,)), ((), ())),
            preferred_element_type=jnp.float32,
        )
        out[columns, :] = jnp.maximum(mixed_rows + bias[...], jnp.float32(0.0)).astype(
            jnp.bfloat16
        )

    def finish(at, code):
        full_copy(at, code, 0, per_dest).wait_send()
        return next_code(at, code)

    lax.fori_loop(0, feats - 1, finish, code)


def per_device(features, tiles, tile_cols, tile_count, send_list, weight, bias):
    blocks, depth, edge = tiles.shape[:3]
    width = features.shape[1]
    verts, feats = lax.axis_size("vert"), lax.axis_size("feat")
    cores = 2 if feats % 2 == 0 else 1
    slots = send_list.shape[2]
    per_dest = blocks // feats
    group = min(GROUP, per_dest)
    parts = per_dest // group
    rows = per_dest * edge
    dead = blocks + verts * slots
    chips = feats // cores
    dims = (verts, feats, cores, blocks, depth, edge, width, slots, group)
    held = [
        pltpu.VMEM((dead + 1, width, edge), jnp.bfloat16),
        pltpu.VMEM((width, blocks * edge), jnp.bfloat16),
        pltpu.VMEM((verts, slots, width, edge), jnp.bfloat16),
        pltpu.VMEM((verts, slots, width, edge), jnp.bfloat16),
        pltpu.VMEM((feats - 1, width, rows), jnp.bfloat16),
        pltpu.VMEM((feats, parts, group, depth, edge, edge), jnp.bfloat16),
        pltpu.VMEM((feats * width, rows), jnp.bfloat16),
    ]
    return pl.pallas_call(
        functools.partial(exchange_kernel, dims),
        out_shape=pltpu.VMEM((rows, weight.shape[1]), jnp.bfloat16),
        in_specs=[pl.BlockSpec(memory_space=pltpu.HBM)] * 7,
        out_specs=pl.BlockSpec(memory_space=pltpu.VMEM),
        scratch_shapes=[
            pltpu.SMEM((depth, blocks), jnp.int32),
            pltpu.SMEM((blocks,), jnp.int32),
            pltpu.SMEM(send_list.shape, jnp.int32),
            pltpu.SemaphoreType.DMA((5,)),
            *held,
            pltpu.VMEM(weight.shape, jnp.bfloat16),
            pltpu.VMEM(bias.shape, jnp.float32),
            pltpu.SemaphoreType.DMA,
            pltpu.SemaphoreType.DMA((feats, parts)),
            pltpu.SemaphoreType.DMA((verts,)),
            pltpu.SemaphoreType.DMA((verts,)),
            pltpu.SemaphoreType.DMA((feats - 1,)),
            pltpu.SemaphoreType.DMA((feats,)),
            pltpu.SemaphoreType.REGULAR((chips + 1,)),
            pltpu.SemaphoreType.REGULAR((chips + 1,)),
        ],
        compiler_params=pltpu.CompilerParams(
            collective_id=0, has_side_effects=True, vmem_limit_bytes=60 * 1024 * 1024
        ),
    )(*(pltpu.with_memory_space_constraint(one, pltpu.HBM) for one in (tile_cols.T, tile_count, send_list, features.T, tiles, weight, bias)))


def solution(mesh):
    return jax.shard_map(
        per_device,
        mesh=mesh,
        in_specs=(
            P("vert", "feat"),
            P("vert", None, None, None),
            P("vert", None),
            P("vert"),
            P("vert", None, None),
            P(),
            P(),
        ),
        out_specs=P(("vert", "feat"), None),
        check_vma=False,
    )
```
